32 devices in a mesh: row: 4 (over y, x), col: 8 (over z, core).
Axes of the slice: x: 2, y: 2, z: 4, core: 2. Of those that a mesh axis runs over, the one named last changes fastest.
Arguments:
- gains: float32 [512, 8, 256], P(('row', 'col')), may hold values from -6 to 6
- coherency: bfloat16 [512, 512, 8, 1, 256], P('row', 'col'), may hold values from -6 to 6
- cotangent: bfloat16 [512, 512, 8, 1, 8], P('row', 'col'), may hold values from -0.099609375 to 0.099609375
- flags: int32 [512, 512, 1], P('row', 'col'), may hold values 0 or 1
- station_slot: int32 [512], replicated, may hold values from 0 to 511, as said below
Outputs:
- gain_grad: float32 [512, 8, 256], P(('row', 'col'))
The draws below stay inside these ranges and needn't reach their ends.
Inputs may be any that keep to these rules, and one draw needn't show every extreme that they name: `station_slot`: each station appears in exactly one slot; in every aligned block of 16 consecutive slots the stations lie with 16 different holders, station s being held by the device of index s // 16 in the order of row+col.
All inputs are finite; a program needn't handle non-finite values. No bound on the sum of `flags` on one device may be relied on, other than what follows from the above.
Results may differ from the reference program's by a relative error of at most 0.0003.
Values sent between devices are 32-bit elements; how exact they have to be, the bound alone decides.
A program may use at most 128 MiB of HBM per device.

```python
import jax
import jax.numpy as jnp
from jax import lax

S = 512
GROUPS = 32
SD = 16
DIR = 32
CH = 8
TI = 1


def draw_station_slot(key, part):
    keys = jax.random.split(jax.random.fold_in(key, 17), 3)
    order = jax.random.permutation(keys[0], GROUPS).astype(jnp.int32)
    within = jax.random.randint(keys[1], (GROUPS,), 0, SD).astype(jnp.int32)
    offset = jax.random.randint(keys[2], (GROUPS,), 0, SD).astype(jnp.int32)
    stride = GROUPS // SD
    blocks = jnp.arange(GROUPS, dtype=jnp.int32)[:, None]
    places = jnp.arange(SD, dtype=jnp.int32)[None, :]
    holder = (order[blocks] + places * stride) % GROUPS
    number = (places + within[holder]) % SD
    station = holder * SD + number
    position = (places + offset[blocks]) % SD
    block_ids = jnp.broadcast_to(blocks, (GROUPS, SD))
    filled = jnp.zeros((GROUPS, SD), jnp.int32).at[block_ids, position].set(station)
    return filled.reshape(GROUPS * SD).astype(jnp.int32)


def plant(array, key, low, largest):
    shape = array.shape
    spot = [jax.random.randint(jax.random.fold_in(key, axis), (), 0, shape[axis]) for axis in range(len(shape))]
    array = array.at[tuple(spot)].set(low)
    longest = shape.index(max(shape))
    spot[longest] = (spot[longest] + 1) % shape[longest]
    return array.at[tuple(spot)].set(largest)


def level_of(stream_key, extent, cuts, low, top_value):
    def one(axis_at, blocks):
        heights = jax.random.uniform(jax.random.fold_in(jax.random.fold_in(stream_key, 6), axis_at), (blocks,), jnp.float32, low / len(cuts), top_value / len(cuts))
        return jnp.repeat(jnp.exp(heights), extent[axis_at] // blocks).reshape((-1,) + (1,) * (len(extent) - axis_at - 1))

    gain = one(*cuts[0])
    for cut in cuts[1:]:
        gain = gain * one(*cut)
    return gain


def centred(rng, shape, spread, most, shards=(), held_as=jnp.bfloat16):
    entries = jax.random.normal(rng, shape, jnp.float32) * spread
    if len(shards) > 0:
        entries = level_of(rng, shape, shards, -0.22, 0.18) * entries
    return jnp.clip(entries, min=-most, max=most).astype(held_as)


def setup_inputs(seed: int = 0) -> dict:
    seeds = jax.random.split(jax.random.key(seed), 6)
    return {
        "gains": centred(seeds[0], (S, CH, 8 * DIR), 1.0, 6.0, ((0, 32),), jnp.float32),
        "coherency": centred(seeds[1], (S, S, CH, TI, 8 * DIR), 1.0, 6.0, ((0, 4), (1, 8))),
        "cotangent": centred(seeds[2], (S, S, CH, TI, 8), 0.016, 0.099609375, ((0, 4), (1, 8))),
        "flags": plant((jax.random.randint(seeds[3], (S, S, TI), 0, 4) < 3).astype(jnp.int32), jax.random.fold_in(seeds[3], 1), 0, 1),
        "station_slot": draw_station_slot(jax.random.fold_in(seeds[5], 71), 0),
    }


def complex_product(first, second):
    return (first[0] * second[0] - first[1] * second[1], first[0] * second[1] + first[1] * second[0])


def complex_sum(first, second):
    return (first[0] + second[0], first[1] + second[1])


def conjugate(element):
    return (element[0], -element[1])


def jones_product(first, second):
    return [complex_sum(complex_product(first[2 * row_index], second[column]), complex_product(first[2 * row_index + 1], second[2 + column])) for row_index in (0, 1) for column in (0, 1)]


def hermitian(matrix):
    return [conjugate(matrix[0]), conjugate(matrix[2]), conjugate(matrix[1]), conjugate(matrix[3])]


def as_complex(parts):
    return [(parts[0], parts[1]), (parts[2], parts[3]), (parts[4], parts[5]), (parts[6], parts[7])]


def as_parts(matrix):
    return [number for element in matrix for number in element]


def block_gradients(coherency, cotangent, flags, row_gains, col_gains):
    shape = coherency.shape
    directions = shape[4] // 8
    coherence = coherency.reshape(shape[:4] + (8, directions))
    weight = flags.astype(jnp.float32)[:, :, None, :, None]
    residual = as_complex([cotangent[..., component].astype(jnp.float32)[..., None] * weight for component in range(8)])
    model_parts = as_complex([coherence[..., component, :].astype(jnp.float32) for component in range(8)])
    row_split = row_gains.reshape(row_gains.shape[0], row_gains.shape[1], 8, directions)
    col_split = col_gains.reshape(col_gains.shape[0], col_gains.shape[1], 8, directions)
    row_jones = as_complex([row_split[:, None, :, None, component, :] for component in range(8)])
    col_jones = as_complex([col_split[None, :, :, None, component, :] for component in range(8)])
    outgoing = jones_product(jones_product(residual, col_jones), hermitian(model_parts))
    row_side = jnp.stack([jnp.sum(part, axis=(1, 3)) for part in as_parts(outgoing)], axis=2)
    incoming = jones_product(jones_product(hermitian(residual), row_jones), model_parts)
    col_side = jnp.stack([jnp.sum(part, axis=(0, 3)) for part in as_parts(incoming)], axis=2)
    return row_side.reshape(row_gains.shape), col_side.reshape(col_gains.shape)


def reference(gains, coherency, cotangent, flags, station_slot):
    slot_gains = jnp.take(gains, station_slot, axis=0)
    block_rows = 16
    stations = gains.shape[0]

    def accumulate(totals, block_index):
        start = (block_index * block_rows).astype(jnp.int32)
        coher_rows = lax.dynamic_slice_in_dim(coherency, start, block_rows, 0)
        cotan_rows = lax.dynamic_slice_in_dim(cotangent, start, block_rows, 0)
        flag_rows = lax.dynamic_slice_in_dim(flags, start, block_rows, 0)
        gain_rows = lax.dynamic_slice_in_dim(slot_gains, start, block_rows, 0)
        row_side, col_side = block_gradients(coher_rows, cotan_rows, flag_rows, gain_rows, slot_gains)
        return totals + col_side, row_side

    indices = jnp.arange(stations // block_rows, dtype=jnp.int32)
    col_total, row_blocks = lax.scan(accumulate, jnp.zeros(gains.shape, gains.dtype), indices)
    slot_grad = row_blocks.reshape(gains.shape) + col_total
    return jnp.zeros(gains.shape, gains.dtype).at[station_slot].set(slot_grad)
```

```python
import functools

import jax
import jax.numpy as jnp
from jax import lax
from jax.experimental import pallas as pl
from jax.experimental.pallas import tpu as pltpu
from jax.sharding import PartitionSpec as P


def swap_pairs(values, width, even):
    return jnp.where(even, pltpu.roll(values, 3 * width, 1), pltpu.roll(values, width, 1))


def two_parts(values):
    high = values.astype(jnp.bfloat16)
    return high, (values - high.astype(jnp.float32)).astype(jnp.bfloat16)


def row_weights(gains, width, even, sign):
    lanes = 4 * width
    rows = []
    for b in range(2):
        half = gains[:, b * lanes : (b + 1) * lanes]
        rows += [half, -sign * swap_pairs(half, width, even)]
    tables = []
    for part in two_parts(jnp.concatenate(rows, axis=0)):
        zero = jnp.zeros_like(part)
        tables += [
            jnp.concatenate([part, zero], axis=1),
            jnp.concatenate([zero, part], axis=1),
        ]
    return jnp.concatenate(tables, axis=0)


def col_weights(gains, width, even, sign, group):
    lanes = 4 * width
    blocks = []
    for b in range(2):
        half = gains[:, b * lanes : (b + 1) * lanes]
        other = pltpu.roll(half, 2 * width, 1)
        rows = [[], []]
        for e in range(2):
            twice = jnp.where(group // 2 == e, half, other)
            rows[0].append(sign * twice)
            rows[1].append(swap_pairs(twice, width, even))
        blocks.append(
            jnp.concatenate([jnp.concatenate(row, axis=1) for row in rows], axis=0)
        )
    tables = []
    for part in range(2):
        for b in range(2):
            value = two_parts(blocks[b])[part]
            zero = jnp.zeros_like(value)
            tables += [
                jnp.concatenate([value, zero], axis=1),
                jnp.concatenate([zero, value], axis=1),
            ]
    return jnp.concatenate(tables, axis=0)


def gradient_kernel(
    width, m_ref, g_ref, gt_ref, jr_ref, jc_ref, r_ref, c_ref,
    wr_ref, wc_ref, xr_ref, xa_ref, xb_ref, acc_ref,
):
    block, second, channels, _ = m_ref.shape
    lanes = 4 * width
    depth = g_ref.shape[2]
    pair = xa_ref.shape[0]
    chunk = xa_ref.shape[1] // channels
    chunks = second // chunk
    step = pl.program_id(0)

    lane_f = lax.broadcasted_iota(jnp.int32, (channels, depth), 1) % channels
    sub_f = lax.broadcasted_iota(jnp.int32, (channels, depth), 0)
    diagonal = (lane_f == sub_f).astype(jnp.float32)
    group = lax.broadcasted_iota(jnp.int32, (channels, lanes), 1) // width
    even = group % 2 == 0
    sign = jnp.where(even, 1.0, -1.0)

    @pl.when(step == 0)
    def _():
        acc_ref[...] = jnp.zeros_like(acc_ref)

        def prepare(k, carry):
            wr_ref[k] = row_weights(jc_ref[k], width, even, sign)
            return carry

        lax.fori_loop(0, second, prepare, 0)

    def spread(rows):
        count = rows.shape[0]
        wide = rows[:, None, :] * diagonal[None]
        return wide.reshape(count * channels, depth).astype(jnp.bfloat16)

    def row_products(k, carry):
        xr_ref[k] = jnp.dot(
            spread(gt_ref[k]), wr_ref[k], preferred_element_type=jnp.float32
        )
        return carry

    lax.fori_loop(0, second, row_products, 0, unroll=4)

    def stations(pair_index, carry):
        first = pair_index * pair
        for p in range(pair):
            wc_ref[p] = col_weights(jr_ref[first + p], width, even, sign, group)

        def col_products(at, x_ref):
            start = pl.multiple_of(at * chunk, chunk)
            for p in range(pair):
                x_ref[p] = jnp.dot(
                    spread(g_ref[first + p, pl.ds(start, chunk)]),
                    wc_ref[p],
                    preferred_element_type=jnp.float32,
                )

        def combine(at, x_ref, totals):
            totals = list(totals)
            for q in range(chunk):
                k = at * chunk + q
                col = [acc_ref[k, n] for n in range(4)]
                for p in range(pair):
                    m = m_ref[first + p, k].astype(jnp.float32)
                    halves = [m[:, :lanes], m[:, lanes:]]
                    swapped = [swap_pairs(h, width, even) for h in halves]
                    start = pl.multiple_of((first + p) * channels, channels)
                    for a in range(2):
                        x = xr_ref[k, pl.ds(start, channels), a * lanes : (a + 1) * lanes]
                        for c in range(2):
                            n = p * 8 + 4 * a + 2 * c
                            totals[n] = totals[n] + x * halves[c]
                            totals[n + 1] = totals[n + 1] + x * swapped[c]
                    for a in range(2):
                        for e in range(2):
                            n = 2 * a + e
                            y = x_ref[
                                p,
                                q * channels : (q + 1) * channels,
                                n * lanes : (n + 1) * lanes,
                            ]
                            col[2 * a] = col[2 * a] + y * halves[e]
                            col[2 * a + 1] = col[2 * a + 1] + y * swapped[e]
                for n in range(4):
                    acc_ref[k, n] = col[n]
            return tuple(totals)

        def two_chunks(j, totals):
            col_products(2 * j + 1, xb_ref)
            totals = combine(2 * j, xa_ref, totals)
            col_products(jnp.minimum(2 * j + 2, chunks - 1), xa_ref)
            return combine(2 * j + 1, xb_ref, totals)

        zero = jnp.zeros((channels, lanes), jnp.float32)
        col_products(0, xa_ref)
        totals = lax.fori_loop(0, chunks // 2, two_chunks, (zero,) * (8 * pair))
        for p in range(pair):
            for a in range(2):
                parts = []
                for n in range(4):
                    value = totals[8 * p + 4 * a + n]
                    if n % 2 == 1:
                        value = -sign * value
                    value = value + pltpu.roll(value, 2 * width, 1)
                    parts.append(value + pltpu.roll(value, width, 1))
                r_ref[first + p, :, a * lanes : (a + 1) * lanes] = jnp.where(
                    group < 2,
                    jnp.where(even, parts[0], parts[1]),
                    jnp.where(even, parts[2], parts[3]),
                )
        return carry

    lax.fori_loop(0, block // pair, stations, 0)

    @pl.when(step == pl.num_programs(0) - 1)
    def _():
        def finish(k, carry):
            for a in range(2):
                real = acc_ref[k, 2 * a]
                imag = acc_ref[k, 2 * a + 1] * sign
                real = real + swap_pairs(real, width, even)
                imag = imag + swap_pairs(imag, width, even)
                c_ref[k, :, a * lanes : (a + 1) * lanes] = jnp.where(even, real, imag)
            return carry

        lax.fori_loop(0, second, finish, 0, unroll=2)


def residuals(cotangent, flags):
    first, second, channels = cotangent.shape[:3]
    weighted = cotangent[:, :, :, 0].astype(jnp.float32) * flags.astype(jnp.float32)[..., None]
    lane_order = weighted.transpose(0, 1, 3, 2).reshape(first, second, 8 * channels)
    doubled = jnp.concatenate([lane_order, lane_order], axis=-1)
    return doubled, doubled.transpose(1, 0, 2)


def block_gradients(coherency, doubled, across, row_gains, col_gains):
    first, second, channels, _, wide = coherency.shape
    width = wide // 8
    block = min(16, first)
    pair = 2
    chunk = min(16, second // 2)
    depth = doubled.shape[2]
    model = coherency.reshape(first, second, channels, wide)
    products = (pair, chunk * channels, 2 * wide)
    return pl.pallas_call(
        functools.partial(gradient_kernel, width),
        grid=(first // block,),
        in_specs=[
            pl.BlockSpec((block, second, channels, wide), lambda s: (s, 0, 0, 0)),
            pl.BlockSpec((block, second, depth), lambda s: (s, 0, 0)),
            pl.BlockSpec((second, block, depth), lambda s: (0, s, 0)),
            pl.BlockSpec((block, channels, wide), lambda s: (s, 0, 0)),
            pl.BlockSpec((second, channels, wide), lambda s: (0, 0, 0)),
        ],
        out_specs=[
            pl.BlockSpec((block, channels, wide), lambda s: (s, 0, 0)),
            pl.BlockSpec((second, channels, wide), lambda s: (0, 0, 0)),
        ],
        out_shape=[
            jax.ShapeDtypeStruct((first, channels, wide), jnp.float32),
            jax.ShapeDtypeStruct((second, channels, wide), jnp.float32),
        ],
        scratch_shapes=[
            pltpu.VMEM((second, depth, wide), jnp.bfloat16),
            pltpu.VMEM((pair, depth, 2 * wide), jnp.bfloat16),
            pltpu.VMEM((second, block * channels, wide), jnp.float32),
            pltpu.VMEM(products, jnp.float32),
            pltpu.VMEM(products, jnp.float32),
            pltpu.VMEM((second, 4, channels, wide // 2), jnp.float32),
        ],
        compiler_params=pltpu.CompilerParams(
            dimension_semantics=("arbitrary",), vmem_limit_bytes=58 * 1024 * 1024
        ),
    )(model, doubled, across, row_gains, col_gains)


def selector(identifiers, count):
    return (identifiers[:, None] == jnp.arange(count, dtype=jnp.int32)[None, :]).astype(jnp.float32)


def select_rows(table, values):
    return jnp.dot(
        table, values, precision=lax.Precision.HIGHEST, preferred_element_type=jnp.float32
    )


def shards(gains, coherency, cotangent, flags, station_slot):
    stations = station_slot.shape[0]
    share = gains.shape[0]
    flat = gains.shape[1] * gains.shape[2]
    row_total = lax.axis_size("row")
    col_total = lax.axis_size("col")
    groups = row_total * col_total
    row_place = lax.axis_index("row")
    col_place = lax.axis_index("col")
    device_place = row_place * col_total + col_place
    counting = jnp.arange(share, dtype=jnp.int32)
    slot_of = (
        jnp.zeros((stations,), jnp.int32)
        .at[station_slot]
        .set(jnp.arange(stations, dtype=jnp.int32))
    )
    own_blocks = jnp.take(slot_of, device_place * share + counting) // share
    col_target = own_blocks % row_total * col_total + own_blocks // row_total
    col_block = col_place * row_total + row_place
    row_holder = jnp.take(station_slot, device_place * share + counting) // share
    col_holder = jnp.take(station_slot, col_block * share + counting) // share
    row_count = coherency.shape[0]
    col_count = coherency.shape[1]
    row_ids = lax.dynamic_slice_in_dim(station_slot, row_place * row_count, row_count)
    col_ids = lax.dynamic_slice_in_dim(station_slot, col_place * col_count, col_count)
    every_gain = lax.all_gather(gains, ("row", "col"), axis=0, tiled=True)
    row_gains = jnp.take(every_gain, row_ids, axis=0)
    col_gains = jnp.take(every_gain, col_ids, axis=0)
    row_side, col_side = block_gradients(
        coherency, *residuals(cotangent, flags), row_gains, col_gains
    )
    row_sum = lax.psum_scatter(row_side, "col", scatter_dimension=0, tiled=True)
    col_sum = lax.psum_scatter(col_side, "row", scatter_dimension=0, tiled=True)
    back_row = select_rows(selector(row_holder, groups).T, row_sum.reshape(share, flat))
    back_col = select_rows(selector(col_holder, groups).T, col_sum.reshape(share, flat))
    recv_row, recv_col = (
        lax.all_to_all(back_row, ("row", "col"), split_axis=0, concat_axis=0, tiled=True),
        lax.all_to_all(back_col, ("row", "col"), split_axis=0, concat_axis=0, tiled=True),
    )
    result = select_rows(selector(own_blocks, groups), recv_row) + select_rows(
        selector(col_target, groups), recv_col
    )
    return result.reshape(gains.shape)


def solution(mesh):
    placed = (
        P(("row", "col"), None, None),
        P("row", "col", None, None, None),
        P("row", "col", None, None, None),
        P("row", "col", None),
        P(),
    )
    return jax.shard_map(
        shards, mesh=mesh, in_specs=placed, out_specs=P(("row", "col"), None, None), check_vma=False
    )
```

```python
import functools

import jax
import jax.numpy as jnp
from jax import lax
from jax.experimental import pallas as pl
from jax.experimental.pallas import tpu as pltpu
from jax.sharding import PartitionSpec as P


def swap_pairs(values, width, even):
    return jnp.where(even, pltpu.roll(values, 3 * width, 1), pltpu.roll(values, width, 1))


def two_parts(values):
    high = values.astype(jnp.bfloat16)
    return high, (values - high.astype(jnp.float32)).astype(jnp.bfloat16)


def row_weights(gains, width, even, sign):
    lanes = 4 * width
    rows = []
    for b in range(2):
        half = gains[:, b * lanes : (b + 1) * lanes]
        rows += [half, -sign * swap_pairs(half, width, even)]
    tables = []
    for part in two_parts(jnp.concatenate(rows, axis=0)):
        zero = jnp.zeros_like(part)
        tables += [
            jnp.concatenate([part, zero], axis=1),
            jnp.concatenate([zero, part], axis=1),
        ]
    return jnp.concatenate(tables, axis=0)


def col_weights(gains, width, even, sign, group):
    lanes = 4 * width
    blocks = []
    for b in range(2):
        half = gains[:, b * lanes : (b + 1) * lanes]
        other = pltpu.roll(half, 2 * width, 1)
        rows = [[], []]
        for e in range(2):
            twice = jnp.where(group // 2 == e, half, other)
            rows[0].append(sign * twice)
            rows[1].append(swap_pairs(twice, width, even))
        blocks.append(
            jnp.concatenate([jnp.concatenate(row, axis=1) for row in rows], axis=0)
        )
    tables = []
    for part in range(2):
        for b in range(2):
            value = two_parts(blocks[b])[part]
            zero = jnp.zeros_like(value)
            tables += [
                jnp.concatenate([value, zero], axis=1),
                jnp.concatenate([zero, value], axis=1),
            ]
    return jnp.concatenate(tables, axis=0)


def gradient_kernel(
    width, m_ref, g_ref, gt_ref, jr_ref, jc_ref, r_ref, c_ref,
    wr_ref, wc_ref, xr_ref, xa_ref, xb_ref, acc_ref,
):
    block, second, channels, _ = m_ref.shape
    lanes = 4 * width
    depth = g_ref.shape[2]
    pair = xa_ref.shape[0]
    chunk = xa_ref.shape[1] // channels
    chunks = second // chunk
    step = pl.program_id(0)

    lane_f = lax.broadcasted_iota(jnp.int32, (channels, depth), 1) % channels
    sub_f = lax.broadcasted_iota(jnp.int32, (channels, depth), 0)
    diagonal = (lane_f == sub_f).astype(jnp.float32)
    group = lax.broadcasted_iota(jnp.int32, (channels, lanes), 1) // width
    even = group % 2 == 0
    sign = jnp.where(even, 1.0, -1.0)

    @pl.when(step == 0)
    def _():
        acc_ref[...] = jnp.zeros_like(acc_ref)

        def prepare(k, carry):
            wr_ref[k] = row_weights(jc_ref[k], width, even, sign)
            return carry

        lax.fori_loop(0, second, prepare, 0)

    def spread(rows):
        count = rows.shape[0]
        wide = rows[:, None, :] * diagonal[None]
        return wide.reshape(count * channels, depth).astype(jnp.bfloat16)

    def row_products(k, carry):
        xr_ref[k] = jnp.dot(
            spread(gt_ref[k]), wr_ref[k], preferred_element_type=jnp.float32
        )
        return carry

    lax.fori_loop(0, second, row_products, 0, unroll=4)

    def stations(pair_index, carry):
        first = pair_index * pair
        for p in range(pair):
            wc_ref[p] = col_weights(jr_ref[first + p], width, even, sign, group)

        def col_products(at, x_ref):
            start = pl.multiple_of(at * chunk, chunk)
            for p in range(pair):
                x_ref[p] = jnp.dot(
                    spread(g_ref[first + p, pl.ds(start, chunk)]),
                    wc_ref[p],
                    preferred_element_type=jnp.float32,
                )

        def combine(at, x_ref, totals):
            totals = list(totals)
            for q in range(chunk):
                k = at * chunk + q
                col = [acc_ref[k, n] for n in range(4)]
                for p in range(pair):
                    m = m_ref[first + p, k].astype(jnp.float32)
                    halves = [m[:, :lanes], m[:, lanes:]]
                    swapped = [swap_pairs(h, width, even) for h in halves]
                    start = pl.multiple_of((first + p) * channels, channels)
                    for a in range(2):
                        x = xr_ref[k, pl.ds(start, channels), a * lanes : (a + 1) * lanes]
                        for c in range(2):
                            n = p * 8 + 4 * a + 2 * c
                            totals[n] = totals[n] + x * halves[c]
                            totals[n + 1] = totals[n + 1] + x * swapped[c]
                    for a in range(2):
                        for e in range(2):
                            n = 2 * a + e
                            y = x_ref[
                                p,
                                q * channels : (q + 1) * channels,
                                n * lanes : (n + 1) * lanes,
                            ]
                            col[2 * a] = col[2 * a] + y * halves[e]
                            col[2 * a + 1] = col[2 * a + 1] + y * swapped[e]
                for n in range(4):
                    acc_ref[k, n] = col[n]
            return tuple(totals)

        def two_chunks(j, totals):
            col_products(2 * j + 1, xb_ref)
            totals = combine(2 * j, xa_ref, totals)
            col_products(jnp.minimum(2 * j + 2, chunks - 1), xa_ref)
            return combine(2 * j + 1, xb_ref, totals)

        zero = jnp.zeros((channels, lanes), jnp.float32)
        col_products(0, xa_ref)
        totals = lax.fori_loop(0, chunks // 2, two_chunks, (zero,) * (8 * pair))
        for p in range(pair):
            for a in range(2):
                parts = []
                for n in range(4):
                    value = totals[8 * p + 4 * a + n]
                    if n % 2 == 1:
                        value = -sign * value
                    value = value + pltpu.roll(value, 2 * width, 1)
                    parts.append(value + pltpu.roll(value, width, 1))
                r_ref[first + p, :, a * lanes : (a + 1) * lanes] = jnp.where(
                    group < 2,
                    jnp.where(even, parts[0], parts[1]),
                    jnp.where(even, parts[2], parts[3]),
                )
        return carry

    lax.fori_loop(0, block // pair, stations, 0)

    @pl.when(step == pl.num_programs(0) - 1)
    def _():
        def finish(k, carry):
            for a in range(2):
                real = acc_ref[k, 2 * a]
                imag = acc_ref[k, 2 * a + 1] * sign
                real = real + swap_pairs(real, width, even)
                imag = imag + swap_pairs(imag, width, even)
                c_ref[k, :, a * lanes : (a + 1) * lanes] = jnp.where(even, real, imag)
            return carry

        lax.fori_loop(0, second, finish, 0, unroll=2)


def residuals(cotangent, flags):
    first, second, channels = cotangent.shape[:3]
    weighted = cotangent[:, :, :, 0].astype(jnp.float32) * flags.astype(jnp.float32)[..., None]
    lane_order = weighted.transpose(0, 1, 3, 2).reshape(first, second, 8 * channels)
    doubled = jnp.concatenate([lane_order, lane_order], axis=-1)
    return doubled, doubled.transpose(1, 0, 2)


def block_gradients(coherency, doubled, across, row_gains, col_gains):
    first, second, channels, _, wide = coherency.shape
    width = wide // 8
    block = min(16, first)
    pair = 2
    chunk = min(16, second // 2)
    depth = doubled.shape[2]
    model = coherency.reshape(first, second, channels, wide)
    products = (pair, chunk * channels, 2 * wide)
    return pl.pallas_call(
        functools.partial(gradient_kernel, width),
        grid=(first // block,),
        in_specs=[
            pl.BlockSpec((block, second, channels, wide), lambda s: (s, 0, 0, 0)),
            pl.BlockSpec((block, second, depth), lambda s: (s, 0, 0)),
            pl.BlockSpec((second, block, depth), lambda s: (0, s, 0)),
            pl.BlockSpec((block, channels, wide), lambda s: (s, 0, 0)),
            pl.BlockSpec((second, channels, wide), lambda s: (0, 0, 0)),
        ],
        out_specs=[
            pl.BlockSpec((block, channels, wide), lambda s: (s, 0, 0)),
            pl.BlockSpec((second, channels, wide), lambda s: (0, 0, 0)),
        ],
        out_shape=[
            jax.ShapeDtypeStruct((first, channels, wide), jnp.float32),
            jax.ShapeDtypeStruct((second, channels, wide), jnp.float32),
        ],
        scratch_shapes=[
            pltpu.VMEM((second, depth, wide), jnp.bfloat16),
            pltpu.VMEM((pair, depth, 2 * wide), jnp.bfloat16),
            pltpu.VMEM((second, block * channels, wide), jnp.float32),
            pltpu.VMEM(products, jnp.float32),
            pltpu.VMEM(products, jnp.float32),
            pltpu.VMEM((second, 4, channels, wide // 2), jnp.float32),
        ],
        compiler_params=pltpu.CompilerParams(
            dimension_semantics=("arbitrary",), vmem_limit_bytes=58 * 1024 * 1024
        ),
    )(model, doubled, across, row_gains, col_gains)


MESH = pl.DeviceIdType.MESH


def device(place, col_total):
    return (place // col_total, place % col_total)


def remote(source, target, send_sem, recv_sem, where):
    return pltpu.make_async_remote_copy(
        src_ref=source,
        dst_ref=target,
        send_sem=send_sem,
        recv_sem=recv_sem,
        device_id=where,
        device_id_type=MESH,
    )


def each(start, stop, action):
    def body(index, carry):
        action(index)
        return carry

    lax.fori_loop(start, stop, body, 0)


def greet(me, total, col_total):
    barrier = pltpu.get_barrier_semaphore()

    def hello(offset):
        pl.semaphore_signal(
            barrier,
            inc=1,
            device_id=device(lax.rem(me + offset, total), col_total),
            device_id_type=MESH,
        )

    each(1, total, hello)
    pl.semaphore_wait(barrier, total - 1)


def exchange(send_ref, recv_ref, send_sems, recv_sems, me, total, col_total):
    def copy(offset):
        place = lax.rem(me + offset, total)
        return remote(
            send_ref.at[place],
            recv_ref.at[me],
            send_sems.at[offset],
            recv_sems.at[offset],
            device(place, col_total),
        )

    each(1, total, lambda offset: copy(offset).start())
    recv_ref[me] = send_ref[me]
    each(1, total, lambda offset: copy(offset).wait())


def spread_kernel(
    row_total, col_total, holders_ref, send_ref, row_ref, col_ref,
    recv_ref, x_send, x_recv, c_send, c_recv, a_send, a_recv, b_send, b_recv,
):
    share = holders_ref.shape[1]
    r = lax.axis_index("row")
    c = lax.axis_index("col")
    total = row_total * col_total
    me = r * col_total + c
    greet(me, total, col_total)
    exchange(send_ref, recv_ref, x_send, x_recv, me, total, col_total)

    def choose(j):
        row_ref[c * share + j] = recv_ref[holders_ref[0, j], 0]
        col_ref[r * share + j] = recv_ref[holders_ref[1, j], 1]

    each(0, share, choose)
    half = col_total // 2
    partner = c + 1 - 2 * (c % 2)

    def col_copy(offset):
        block = col_ref.at[pl.ds(r * share, share)]
        where = (lax.rem(r + offset, row_total), c)
        return remote(block, block, c_send.at[offset], c_recv.at[offset], where)

    def far_copy(offset):
        block = row_ref.at[pl.ds(c * share, share)]
        where = (r, lax.rem(c + 2 * offset, col_total))
        return remote(block, block, a_send.at[offset], a_recv.at[offset], where)

    def near_copy(offset):
        origin = lax.rem(c + col_total - 2 * offset, col_total)
        block = row_ref.at[pl.ds(origin * share, share)]
        return remote(block, block, b_send.at[offset], b_recv.at[offset], (r, partner))

    each(1, half, lambda offset: far_copy(offset).start())
    each(1, row_total, lambda offset: col_copy(offset).start())
    near_copy(0).start()

    def forward(offset):
        far_copy(offset).wait_recv()
        near_copy(offset).start()

    each(1, half, forward)
    each(1, half, lambda offset: far_copy(offset).wait_send())
    each(0, half, lambda offset: near_copy(offset).wait())
    each(1, row_total, lambda offset: col_copy(offset).wait())


def collect_kernel(
    row_total, col_total, back_ref, own_ref, row_ref, col_ref, out_ref,
    pair_ref, part_ref, far_ref, colin_ref, sums_ref, send_ref, recv_ref,
    x_send, x_recv, c_send, c_recv, a_send, a_recv, b_send, b_recv,
):
    share = own_ref.shape[1]
    r = lax.axis_index("row")
    c = lax.axis_index("col")
    total = row_total * col_total
    me = r * col_total + c
    half = col_total // 2
    core = c % 2
    chip = c // 2
    greet(me, total, col_total)

    def near_copy(offset):
        q = lax.rem(chip + offset, half)
        block = row_ref.at[pl.ds((2 * q + 1 - core) * share, share)]
        return remote(
            block, pair_ref.at[q], a_send.at[offset], a_recv.at[offset], (r, 2 * chip + 1 - core)
        )

    def far_copy(offset):
        q = lax.rem(chip + offset, half)
        return remote(
            part_ref.at[q], far_ref.at[offset], b_send.at[offset], b_recv.at[offset],
            (r, 2 * q + core),
        )

    def col_copy(offset):
        there = lax.rem(r + offset, row_total)
        block = col_ref.at[pl.ds(there * share, share)]
        return remote(
            block, colin_ref.at[offset], c_send.at[offset], c_recv.at[offset], (there, c)
        )

    def join(offset):
        near_copy(offset).wait_recv()
        q = lax.rem(chip + offset, half)
        part_ref[q] = row_ref[pl.ds((2 * q + core) * share, share)] + pair_ref[q]

    def join_and_send(offset):
        join(offset)
        far_copy(offset).start()

    each(1, half + 1, lambda offset: near_copy(lax.rem(offset, half)).start())
    each(1, row_total, lambda offset: col_copy(offset).start())
    each(1, half, join_and_send)
    join(0)
    sums_ref[0] = part_ref[chip]
    sums_ref[1] = col_ref[pl.ds(r * share, share)]

    def add_col(offset):
        col_copy(offset).wait()
        sums_ref[1] += colin_ref[offset]

    def add_row(offset):
        far_copy(offset).wait()
        sums_ref[0] += far_ref[offset]

    each(1, row_total, add_col)
    each(1, half, add_row)
    each(0, half, lambda offset: near_copy(offset).wait_send())

    def address(place):
        send_ref[place, 0] = sums_ref[0, back_ref[0, place]]
        send_ref[place, 1] = sums_ref[1, back_ref[1, place]]

    each(0, total, address)
    exchange(send_ref, recv_ref, x_send, x_recv, me, total, col_total)

    def settle(j):
        out_ref[j] = recv_ref[own_ref[0, j], 0] + recv_ref[own_ref[1, j], 1]

    each(0, share, settle)


def semaphores(total, row_total, col_total):
    counts = (total, row_total, col_total // 2, col_total // 2)
    return [pltpu.SemaphoreType.DMA((count,)) for count in counts for _ in range(2)]


def places(identifiers, count):
    here = identifiers[:, None] == jnp.arange(count, dtype=jnp.int32)[None, :]
    index = jnp.arange(identifiers.shape[0], dtype=jnp.int32)[:, None]
    return jnp.sum(jnp.where(here, index, 0), axis=0, dtype=jnp.int32)


def call_options(identifier):
    return pltpu.CompilerParams(collective_id=identifier, has_side_effects=True)


def shards(gains, coherency, cotangent, flags, station_slot):
    stations = station_slot.shape[0]
    share = gains.shape[0]
    tail = gains.shape[1:]
    row_total = lax.axis_size("row")
    col_total = lax.axis_size("col")
    groups = row_total * col_total
    row_place = lax.axis_index("row")
    col_place = lax.axis_index("col")
    device_place = row_place * col_total + col_place
    counting = jnp.arange(share, dtype=jnp.int32)
    mine = device_place * share + counting
    found = station_slot[None, :] == mine[:, None]
    slot_index = jnp.arange(stations, dtype=jnp.int32)[None, :]
    own_blocks = jnp.sum(jnp.where(found, slot_index, 0), axis=1, dtype=jnp.int32) // share
    col_target = own_blocks % row_total * col_total + own_blocks // row_total
    col_block = col_place * row_total + row_place
    row_holder = lax.dynamic_slice_in_dim(station_slot, device_place * share, share) // share
    col_holder = lax.dynamic_slice_in_dim(station_slot, col_block * share, share) // share
    holders = jnp.stack([row_holder, col_holder])
    targets = jnp.stack([own_blocks, col_target])
    picks = jnp.stack([places(own_blocks, groups), places(col_target, groups)], axis=1)
    sent = jnp.take(gains, picks.reshape(-1), axis=0).reshape((groups, 2) + tail)
    vmem = pl.BlockSpec(memory_space=pltpu.VMEM)
    smem = pl.BlockSpec(memory_space=pltpu.SMEM)
    f32 = jnp.float32
    table = pltpu.VMEM((groups, 2) + tail, f32)
    row_gains, col_gains = pl.pallas_call(
        functools.partial(spread_kernel, row_total, col_total),
        in_specs=[smem, vmem],
        out_specs=[vmem, vmem],
        out_shape=[
            jax.ShapeDtypeStruct((col_total * share,) + tail, f32),
            jax.ShapeDtypeStruct((row_total * share,) + tail, f32),
        ],
        scratch_shapes=[table] + semaphores(groups, row_total, col_total),
        compiler_params=call_options(1),
    )(holders, sent)
    row_side, col_side = block_gradients(
        coherency, *residuals(cotangent, flags), row_gains, col_gains
    )
    backs = jnp.stack([places(row_holder, groups), places(col_holder, groups)])
    half = col_total // 2
    return pl.pallas_call(
        functools.partial(collect_kernel, row_total, col_total),
        in_specs=[smem, smem, vmem, vmem],
        out_specs=vmem,
        out_shape=jax.ShapeDtypeStruct(gains.shape, f32),
        scratch_shapes=[
            pltpu.VMEM((half, share) + tail, f32),
            pltpu.VMEM((half, share) + tail, f32),
            pltpu.VMEM((half, share) + tail, f32),
            pltpu.VMEM((row_total, share) + tail, f32),
            pltpu.VMEM((2, share) + tail, f32),
            table,
            table,
        ]
        + semaphores(groups, row_total, col_total),
        compiler_params=call_options(2),
    )(backs, targets, row_side, col_side)


def solution(mesh):
    placed = (
        P(("row", "col"), None, None),
        P("row", "col", None, None, None),
        P("row", "col", None, None, None),
        P("row", "col", None),
        P(),
    )
    return jax.shard_map(
        shards, mesh=mesh, in_specs=placed, out_specs=P(("row", "col"), None, None), check_vma=False
    )
```

```python
import functools

import jax
import jax.numpy as jnp
from jax import lax
from jax.experimental import pallas as pl
from jax.experimental.pallas import tpu as pltpu
from jax.sharding import PartitionSpec as P


def swap_pairs(values, width, even):
    return jnp.where(even, pltpu.roll(values, 3 * width, 1), pltpu.roll(values, width, 1))


def two_parts(values):
    high = values.astype(jnp.bfloat16)
    return high, (values - high.astype(jnp.float32)).astype(jnp.bfloat16)


def row_weights(gains, width, even, sign):
    lanes = 4 * width
    rows = []
    for b in range(2):
        half = gains[:, b * lanes : (b + 1) * lanes]
        rows += [half, -sign * swap_pairs(half, width, even)]
    tables = []
    for part in two_parts(jnp.concatenate(rows, axis=0)):
        zero = jnp.zeros_like(part)
        tables += [
            jnp.concatenate([part, zero], axis=1),
            jnp.concatenate([zero, part], axis=1),
        ]
    return jnp.concatenate(tables, axis=0)


def col_weights(gains, width, even, sign, group):
    lanes = 4 * width
    blocks = []
    for b in range(2):
        half = gains[:, b * lanes : (b + 1) * lanes]
        other = pltpu.roll(half, 2 * width, 1)
        rows = [[], []]
        for e in range(2):
            twice = jnp.where(group // 2 == e, half, other)
            rows[0].append(sign * twice)
            rows[1].append(swap_pairs(twice, width, even))
        blocks.append(
            jnp.concatenate([jnp.concatenate(row, axis=1) for row in rows], axis=0)
        )
    tables = []
    for part in range(2):
        for b in range(2):
            value = two_parts(blocks[b])[part]
            zero = jnp.zeros_like(value)
            tables += [
                jnp.concatenate([value, zero], axis=1),
                jnp.concatenate([zero, value], axis=1),
            ]
    return jnp.concatenate(tables, axis=0)


def gradient_kernel(
    width, m_ref, gt_ref, jr_ref, jc_ref, r_ref, c_ref,
    wr_ref, wc_ref, xr_ref, xa_ref, xb_ref, acc_ref,
):
    block, second, channels, _ = m_ref.shape
    lanes = 4 * width
    depth = gt_ref.shape[2]
    pair = xa_ref.shape[0]
    chunk = xa_ref.shape[1] // channels
    chunks = second // chunk
    step = pl.program_id(0)

    lane_f = lax.broadcasted_iota(jnp.int32, (channels, depth), 1) % channels
    sub_f = lax.broadcasted_iota(jnp.int32, (channels, depth), 0)
    diagonal = (lane_f == sub_f).astype(jnp.float32)
    group = lax.broadcasted_iota(jnp.int32, (channels, lanes), 1) // width
    even = group % 2 == 0
    sign = jnp.where(even, 1.0, -1.0)

    @pl.when(step == 0)
    def _():
        acc_ref[...] = jnp.zeros_like(acc_ref)

        def prepare(k, carry):
            wr_ref[k] = row_weights(jc_ref[k], width, even, sign)
            return carry

        lax.fori_loop(0, second, prepare, 0)

    def spread(rows):
        count = rows.shape[0]
        wide = rows * diagonal[None]
        return wide.reshape(count * channels, depth).astype(jnp.bfloat16)

    def row_products(k, carry):
        xr_ref[k] = jnp.dot(
            spread(gt_ref[k][:, None, :]), wr_ref[k], preferred_element_type=jnp.float32
        )
        return carry

    lax.fori_loop(0, second, row_products, 0, unroll=4)

    def stations(pair_index, carry):
        first = pair_index * pair
        for p in range(pair):
            wc_ref[p] = col_weights(jr_ref[first + p], width, even, sign, group)

        def col_products(at, x_ref):
            start = pl.multiple_of(at * chunk, chunk)
            for p in range(pair):
                x_ref[p] = jnp.dot(
                    spread(gt_ref[pl.ds(start, chunk), pl.ds(first + p, 1)]),
                    wc_ref[p],
                    preferred_element_type=jnp.float32,
                )

        def combine(at, x_ref, totals):
            totals = list(totals)
            for q in range(chunk):
                k = at * chunk + q
                col = [acc_ref[k, n] for n in range(4)]
                for p in range(pair):
                    m = m_ref[first + p, k].astype(jnp.float32)
                    halves = [m[:, :lanes], m[:, lanes:]]
                    swapped = [swap_pairs(h, width, even) for h in halves]
                    start = pl.multiple_of((first + p) * channels, channels)
                    for a in range(2):
                        x = xr_ref[k, pl.ds(start, channels), a * lanes : (a + 1) * lanes]
                        for c in range(2):
                            n = p * 8 + 4 * a + 2 * c
                            totals[n] = totals[n] + x * halves[c]
                            totals[n + 1] = totals[n + 1] + x * swapped[c]
                    for a in range(2):
                        for e in range(2):
                            n = 2 * a + e
                            y = x_ref[
                                p,
                                q * channels : (q + 1) * channels,
                                n * lanes : (n + 1) * lanes,
                            ]
                            col[2 * a] = col[2 * a] + y * halves[e]
                            col[2 * a + 1] = col[2 * a + 1] + y * swapped[e]
                for n in range(4):
                    acc_ref[k, n] = col[n]
            return tuple(totals)

        def two_chunks(j, totals):
            col_products(2 * j + 1, xb_ref)
            totals = combine(2 * j, xa_ref, totals)
            col_products(jnp.minimum(2 * j + 2, chunks - 1), xa_ref)
            return combine(2 * j + 1, xb_ref, totals)

        zero = jnp.zeros((channels, lanes), jnp.float32)
        col_products(0, xa_ref)
        totals = lax.fori_loop(0, chunks // 2, two_chunks, (zero,) * (8 * pair))
        for p in range(pair):
            for a in range(2):
                parts = []
                for n in range(4):
                    value = totals[8 * p + 4 * a + n]
                    if n % 2 == 1:
                        value = -sign * value
                    value = value + pltpu.roll(value, 2 * width, 1)
                    parts.append(value + pltpu.roll(value, width, 1))
                r_ref[first + p, :, a * lanes : (a + 1) * lanes] = jnp.where(
                    group < 2,
                    jnp.where(even, parts[0], parts[1]),
                    jnp.where(even, parts[2], parts[3]),
                )
        return carry

    lax.fori_loop(0, block // pair, stations, 0)

    @pl.when(step == pl.num_programs(0) - 1)
    def _():
        def finish(k, carry):
            for a in range(2):
                real = acc_ref[k, 2 * a]
                imag = acc_ref[k, 2 * a + 1] * sign
                real = real + swap_pairs(real, width, even)
                imag = imag + swap_pairs(imag, width, even)
                c_ref[k, :, a * lanes : (a + 1) * lanes] = jnp.where(even, real, imag)
            return carry

        lax.fori_loop(0, second, finish, 0, unroll=2)


def residuals(cotangent, flags):
    first, second, channels = cotangent.shape[:3]
    weighted = cotangent[:, :, :, 0].astype(jnp.float32) * flags.astype(jnp.float32)[..., None]
    lane_order = weighted.transpose(1, 0, 3, 2).reshape(second, first, 8 * channels)
    return jnp.concatenate([lane_order, lane_order], axis=-1)


def block_gradients(coherency, across, row_gains, col_gains):
    first, second, channels, _, wide = coherency.shape
    width = wide // 8
    block = min(32, first)
    pair = 2
    chunk = min(16, second // 2)
    depth = across.shape[2]
    model = coherency.reshape(first, second, channels, wide)
    products = (pair, chunk * channels, 2 * wide)
    return pl.pallas_call(
        functools.partial(gradient_kernel, width),
        grid=(first // block,),
        in_specs=[
            pl.BlockSpec((block, second, channels, wide), lambda s: (s, 0, 0, 0)),
            pl.BlockSpec((second, block, depth), lambda s: (0, s, 0)),
            pl.BlockSpec((block, channels, wide), lambda s: (s, 0, 0)),
            pl.BlockSpec((second, channels, wide), lambda s: (0, 0, 0)),
        ],
        out_specs=[
            pl.BlockSpec((block, channels, wide), lambda s: (s, 0, 0)),
            pl.BlockSpec((second, channels, wide), lambda s: (0, 0, 0)),
        ],
        out_shape=[
            jax.ShapeDtypeStruct((first, channels, wide), jnp.float32),
            jax.ShapeDtypeStruct((second, channels, wide), jnp.float32),
        ],
        scratch_shapes=[
            pltpu.VMEM((second, depth, wide), jnp.bfloat16),
            pltpu.VMEM((pair, depth, 2 * wide), jnp.bfloat16),
            pltpu.VMEM((second, block * channels, wide), jnp.float32),
            pltpu.VMEM(products, jnp.float32),
            pltpu.VMEM(products, jnp.float32),
            pltpu.VMEM((second, 4, channels, wide // 2), jnp.float32),
        ],
        compiler_params=pltpu.CompilerParams(
            dimension_semantics=("arbitrary",), vmem_limit_bytes=58 * 1024 * 1024
        ),
    )(model, across, row_gains, col_gains)


MESH = pl.DeviceIdType.MESH


def device(place, col_total):
    return (place // col_total, place % col_total)


def remote(source, target, send_sem, recv_sem, where):
    return pltpu.make_async_remote_copy(
        src_ref=source,
        dst_ref=target,
        send_sem=send_sem,
        recv_sem=recv_sem,
        device_id=where,
        device_id_type=MESH,
    )


def each(start, stop, action):
    def body(index, carry):
        action(index)
        return carry

    lax.fori_loop(start, stop, body, 0)


def greet(me, total, col_total):
    barrier = pltpu.get_barrier_semaphore()

    def hello(offset):
        pl.semaphore_signal(
            barrier,
            inc=1,
            device_id=device(lax.rem(me + offset, total), col_total),
            device_id_type=MESH,
        )

    each(1, total, hello)
    pl.semaphore_wait(barrier, total - 1)


def exchange(send_ref, recv_ref, send_sems, recv_sems, me, total, col_total):
    def copy(offset):
        place = lax.rem(me + offset, total)
        return remote(
            send_ref.at[place],
            recv_ref.at[me],
            send_sems.at[offset],
            recv_sems.at[offset],
            device(place, col_total),
        )

    each(1, total, lambda offset: copy(offset).start())
    recv_ref[me] = send_ref[me]
    each(1, total, lambda offset: copy(offset).wait())


def spread_kernel(
    row_total, col_total, holders_ref, send_ref, row_ref, col_ref,
    recv_ref, x_send, x_recv, c_send, c_recv, a_send, a_recv, b_send, b_recv,
):
    share = holders_ref.shape[1]
    r = lax.axis_index("row")
    c = lax.axis_index("col")
    total = row_total * col_total
    me = r * col_total + c
    greet(me, total, col_total)
    exchange(send_ref, recv_ref, x_send, x_recv, me, total, col_total)

    def choose(j):
        row_ref[c * share + j] = recv_ref[holders_ref[0, j], 0]
        col_ref[r * share + j] = recv_ref[holders_ref[1, j], 1]

    each(0, share, choose)
    half = col_total // 2
    partner = c + 1 - 2 * (c % 2)

    def col_copy(offset):
        block = col_ref.at[pl.ds(r * share, share)]
        where = (lax.rem(r + offset, row_total), c)
        return remote(block, block, c_send.at[offset], c_recv.at[offset], where)

    def far_copy(offset):
        block = row_ref.at[pl.ds(c * share, share)]
        where = (r, lax.rem(c + 2 * offset, col_total))
        return remote(block, block, a_send.at[offset], a_recv.at[offset], where)

    def near_copy(offset):
        origin = lax.rem(c + col_total - 2 * offset, col_total)
        block = row_ref.at[pl.ds(origin * share, share)]
        return remote(block, block, b_send.at[offset], b_recv.at[offset], (r, partner))

    each(1, half, lambda offset: far_copy(offset).start())
    each(1, row_total, lambda offset: col_copy(offset).start())
    near_copy(0).start()

    def forward(offset):
        far_copy(offset).wait_recv()
        near_copy(offset).start()

    each(1, half, forward)
    each(1, half, lambda offset: far_copy(offset).wait_send())
    each(0, half, lambda offset: near_copy(offset).wait())
    each(1, row_total, lambda offset: col_copy(offset).wait())


def collect_kernel(
    row_total, col_total, back_ref, own_ref, row_ref, col_ref, out_ref,
    pair_ref, part_ref, far_ref, colin_ref, sums_ref, send_ref, recv_ref,
    x_send, x_recv, c_send, c_recv, a_send, a_recv, b_send, b_recv,
):
    share = own_ref.shape[1]
    r = lax.axis_index("row")
    c = lax.axis_index("col")
    total = row_total * col_total
    me = r * col_total + c
    half = col_total // 2
    core = c % 2
    chip = c // 2
    greet(me, total, col_total)

    def near_copy(offset):
        q = lax.rem(chip + offset, half)
        block = row_ref.at[pl.ds((2 * q + 1 - core) * share, share)]
        return remote(
            block, pair_ref.at[q], a_send.at[offset], a_recv.at[offset], (r, 2 * chip + 1 - core)
        )

    def far_copy(offset):
        q = lax.rem(chip + offset, half)
        return remote(
            part_ref.at[q], far_ref.at[offset], b_send.at[offset], b_recv.at[offset],
            (r, 2 * q + core),
        )

    def col_copy(offset):
        there = lax.rem(r + offset, row_total)
        block = col_ref.at[pl.ds(there * share, share)]
        return remote(
            block, colin_ref.at[offset], c_send.at[offset], c_recv.at[offset], (there, c)
        )

    def join(offset):
        near_copy(offset).wait_recv()
        q = lax.rem(chip + offset, half)
        part_ref[q] = row_ref[pl.ds((2 * q + core) * share, share)] + pair_ref[q]

    def join_and_send(offset):
        join(offset)
        far_copy(offset).start()

    each(1, half + 1, lambda offset: near_copy(lax.rem(offset, half)).start())
    each(1, row_total, lambda offset: col_copy(offset).start())
    each(1, half, join_and_send)
    join(0)
    sums_ref[0] = part_ref[chip]
    sums_ref[1] = col_ref[pl.ds(r * share, share)]

    def add_col(offset):
        col_copy(offset).wait()
        sums_ref[1] += colin_ref[offset]

    def add_row(offset):
        far_copy(offset).wait()
        sums_ref[0] += far_ref[offset]

    each(1, row_total, add_col)
    each(1, half, add_row)
    each(0, half, lambda offset: near_copy(offset).wait_send())

    def address(place):
        send_ref[place, 0] = sums_ref[0, back_ref[0, place]]
        send_ref[place, 1] = sums_ref[1, back_ref[1, place]]

    each(0, total, address)
    exchange(send_ref, recv_ref, x_send, x_recv, me, total, col_total)

    def settle(j):
        out_ref[j] = recv_ref[own_ref[0, j], 0] + recv_ref[own_ref[1, j], 1]

    each(0, share, settle)


def semaphores(total, row_total, col_total):
    counts = (total, row_total, col_total // 2, col_total // 2)
    return [pltpu.SemaphoreType.DMA((count,)) for count in counts for _ in range(2)]


def places(identifiers, count):
    here = identifiers[:, None] == jnp.arange(count, dtype=jnp.int32)[None, :]
    index = jnp.arange(identifiers.shape[0], dtype=jnp.int32)[:, None]
    return jnp.sum(jnp.where(here, index, 0), axis=0, dtype=jnp.int32)


def call_options(identifier):
    return pltpu.CompilerParams(collective_id=identifier, has_side_effects=True)


def shards(gains, coherency, cotangent, flags, station_slot):
    stations = station_slot.shape[0]
    share = gains.shape[0]
    tail = gains.shape[1:]
    row_total = lax.axis_size("row")
    col_total = lax.axis_size("col")
    groups = row_total * col_total
    row_place = lax.axis_index("row")
    col_place = lax.axis_index("col")
    device_place = row_place * col_total + col_place
    counting = jnp.arange(share, dtype=jnp.int32)
    mine = device_place * share + counting
    found = station_slot[None, :] == mine[:, None]
    slot_index = jnp.arange(stations, dtype=jnp.int32)[None, :]
    own_blocks = jnp.sum(jnp.where(found, slot_index, 0), axis=1, dtype=jnp.int32) // share
    col_target = own_blocks % row_total * col_total + own_blocks // row_total
    col_block = col_place * row_total + row_place
    row_holder = lax.dynamic_slice_in_dim(station_slot, device_place * share, share) // share
    col_holder = lax.dynamic_slice_in_dim(station_slot, col_block * share, share) // share
    holders = jnp.stack([row_holder, col_holder])
    targets = jnp.stack([own_blocks, col_target])
    picks = jnp.stack([places(own_blocks, groups), places(col_target, groups)], axis=1)
    sent = jnp.take(gains, picks.reshape(-1), axis=0).reshape((groups, 2) + tail)
    vmem = pl.BlockSpec(memory_space=pltpu.VMEM)
    smem = pl.BlockSpec(memory_space=pltpu.SMEM)
    f32 = jnp.float32
    table = pltpu.VMEM((groups, 2) + tail, f32)
    row_gains, col_gains = pl.pallas_call(
        functools.partial(spread_kernel, row_total, col_total),
        in_specs=[smem, vmem],
        out_specs=[vmem, vmem],
        out_shape=[
            jax.ShapeDtypeStruct((col_total * share,) + tail, f32),
            jax.ShapeDtypeStruct((row_total * share,) + tail, f32),
        ],
        scratch_shapes=[table] + semaphores(groups, row_total, col_total),
        compiler_params=call_options(1),
    )(holders, sent)
    row_side, col_side = block_gradients(
        coherency, residuals(cotangent, flags), row_gains, col_gains
    )
    backs = jnp.stack([places(row_holder, groups), places(col_holder, groups)])
    half = col_total // 2
    return pl.pallas_call(
        functools.partial(collect_kernel, row_total, col_total),
        in_specs=[smem, smem, vmem, vmem],
        out_specs=vmem,
        out_shape=jax.ShapeDtypeStruct(gains.shape, f32),
        scratch_shapes=[
            pltpu.VMEM((half, share) + tail, f32),
            pltpu.VMEM((half, share) + tail, f32),
            pltpu.VMEM((half, share) + tail, f32),
            pltpu.VMEM((row_total, share) + tail, f32),
            pltpu.VMEM((2, share) + tail, f32),
            table,
            table,
        ]
        + semaphores(groups, row_total, col_total),
        compiler_params=call_options(2),
    )(backs, targets, row_side, col_side)


def solution(mesh):
    placed = (
        P(("row", "col"), None, None),
        P("row", "col", None, None, None),
        P("row", "col", None, None, None),
        P("row", "col", None),
        P(),
    )
    return jax.shard_map(
        shards, mesh=mesh, in_specs=placed, out_specs=P(("row", "col"), None, None), check_vma=False
    )
```
